32 devices in a mesh: grp: 2 (over y), row: 16 (over z, x, core).
Axes of the slice: x: 2, y: 2, z: 4, core: 2. Of those that a mesh axis runs over, the one named last changes fastest.
Arguments:
- queries: bfloat16 [4096, 4096], P(('grp', 'row')), parts along dimension 0, may hold values from -130 to 130
- answer_keys: bfloat16 [4096, 512], P(('grp', 'row')), parts along dimension 0, may hold values from -6 to 6
- answer_values: bfloat16 [4096, 512], P(('grp', 'row')), parts along dimension 0, may hold values from -6 to 6
- prompt_keys: bfloat16 [256, 512], P(('grp', 'row')), parts along dimension 0, may hold values from -4 to 4
- prompt_values: bfloat16 [256, 512], P(('grp', 'row')), parts along dimension 0, may hold values from -6 to 6
- out_grad: bfloat16 [4096, 4096], P(('grp', 'row')), parts along dimension 0, may hold values from -6 to 6
- weights: float32 [4096], P(('grp', 'row')), parts along dimension 0, may hold values from 0.25 to 4
- lengths: int32 [64], P('grp'), parts along dimension 0, may hold values from 1 to 256, as said below
Outputs:
- attn_out: bfloat16 [4096, 4096], P(('grp', 'row')), parts along dimension 0
- q_grad: bfloat16 [4096, 4096], P(('grp', 'row')), parts along dimension 0
- answer_key_grad: bfloat16 [4096, 512], P(('grp', 'row')), parts along dimension 0
- answer_value_grad: bfloat16 [4096, 512], P(('grp', 'row')), parts along dimension 0
- prompt_key_grad: float32 [256, 512], P(('grp', 'row')), parts along dimension 0
- prompt_value_grad: float32 [256, 512], P(('grp', 'row')), parts along dimension 0
The draws below stay inside these ranges and needn't reach their ends.
There are 2 independent parts, one for each index of `grp`. The reference program is written for one: setup_inputs(seed, part) draws one part's arguments, and reference() takes and returns one part's arrays. A program takes and returns all parts, laid end to end along the dimension named above; each array names one. Nothing has to cross between parts.
Inputs may be any that keep to these rules, and one draw needn't show every extreme that they name: `lengths`: the answers fill the 2048 packed rows in order; the longest has exactly 256 rows.
All inputs are finite; a program needn't handle non-finite values.
Results may differ from the reference program's by a relative error of at most 0.02.
Values may be sent and summed in bfloat16 or wider, within the bound.
A program may use at most 192 MiB of HBM per device.

```python
import math
import jax
import jax.numpy as jnp
from jax import lax

HEADS = 32
KV_HEADS = 4
HEAD_DIM = 128
ROWS_DEV = 128
ROWS = 2048
PROMPT = 128
ANSWERS = 32
MOST_LEN = 256
N_ROW = 16


def drawn_pair(key):
    folded = jax.random.fold_in(key, 11)
    key_draw, query_draw = jax.random.split(folded, 2)
    prompt_rows = jnp.clip(jax.random.normal(key_draw, (PROMPT, KV_HEADS * HEAD_DIM), jnp.float32), -4.0, 4.0)
    queries = jnp.clip(3.0 * jax.random.normal(query_draw, (ROWS, HEADS * HEAD_DIM), jnp.float32), -18.0, 18.0)
    return (queries, prompt_rows)


def draw_queries(key, part):
    return drawn_pair(key)[0].astype(jnp.bfloat16)


def draw_prompt_keys(key, part):
    return drawn_pair(key)[1].astype(jnp.bfloat16)


def draw_lengths(key, part):
    total = ROWS - MOST_LEN - 1
    count = ANSWERS - 2
    height = MOST_LEN // 2
    spots = jnp.arange(1, total, dtype=jnp.int32)
    order = jax.random.permutation(jax.random.fold_in(key, 23), total - 1).astype(jnp.int32)
    inside = spots % height
    ranking = jnp.where(inside == height // 2, -1, jnp.where(inside == 0, total + order, order))
    picked = jnp.argsort(ranking, stable=True)[:count - 1]
    cuts = jnp.sort(spots[picked])
    edges = jnp.concatenate([jnp.zeros((1,), jnp.int32), cuts, jnp.full((1,), total, jnp.int32)])
    leading = edges[1:] - edges[:-1]
    closing = jnp.array([MOST_LEN, 1], dtype=jnp.int32)
    return jnp.concatenate([leading, closing]).astype(jnp.int32)


def block_levels(rng, dims, shards, least, largest):
    factor_of, own = 1.0, jax.random.fold_in(rng, 6)
    for axis_at, shards_of in shards:
        steps = jnp.exp(jax.random.uniform(jax.random.fold_in(own, axis_at), (shards_of,), jnp.float32, least / len(shards), largest / len(shards)))
        factor_of = factor_of * jnp.repeat(steps, dims[axis_at] // shards_of).reshape([-1 if axis == axis_at else 1 for axis in range(len(dims))])
    return factor_of


def scatter_about(key, extent, scale, bound, pieces=(), held_as=jnp.bfloat16):
    loudness = block_levels(key, extent, pieces, -0.22, 0.18) if pieces else 1.0
    values = jax.random.normal(key, extent, jnp.float32) * scale * loudness
    return jnp.minimum(jnp.maximum(values, -bound), bound).astype(held_as)


def setup_inputs(seed: int = 0, part: int = 0) -> dict:
    seeds = jax.random.split(jax.random.key(seed), 9)
    part_splits = jax.random.split(jax.random.fold_in(seeds[8], part), 9)
    return {
        "queries": draw_queries(jax.random.fold_in(jax.random.fold_in(seeds[8], part), 71), part),
        "answer_keys": scatter_about(part_splits[1], (ROWS, KV_HEADS * HEAD_DIM), 1.0, 6.0, ((0, 16),)),
        "answer_values": scatter_about(part_splits[2], (ROWS, KV_HEADS * HEAD_DIM), 1.0, 6.0, ((0, 16),)),
        "prompt_keys": draw_prompt_keys(jax.random.fold_in(jax.random.fold_in(seeds[8], part), 71), part),
        "prompt_values": scatter_about(part_splits[4], (PROMPT, KV_HEADS * HEAD_DIM), 1.0, 6.0, ((0, 16),)),
        "out_grad": scatter_about(part_splits[5], (ROWS, HEADS * HEAD_DIM), 1.0, 6.0, ((0, 16),)),
        "weights": jnp.clip(jnp.exp(math.log(4.0) - 2.7725887 * jax.random.uniform(part_splits[6], (ROWS,), jnp.float32) ** block_levels(part_splits[6], (ROWS,), ((0, 16),), -0.2, 0.2)), 0.25, 4.0),
        "lengths": draw_lengths(jax.random.fold_in(jax.random.fold_in(seeds[8], part), 71), part),
    }


MASKED = -1.0e30


def times_transposed(former, latter):
    return lax.dot_general(former, latter, (((1,), (1,)), ((), ())), preferred_element_type=jnp.float32)


def transposed_times(former, latter):
    return lax.dot_general(former, latter, (((0,), (0,)), ((), ())), preferred_element_type=jnp.float32)


def segment_of(positions, lengths):
    finish = jnp.cumsum(lengths, dtype=jnp.int32)
    starts = finish - lengths
    covered = (starts[None, :] <= positions[:, None]).astype(jnp.int32)
    return jnp.sum(covered, axis=1, dtype=jnp.int32) - 1


def probabilities(flat_queries, key_rows, allowed, group_size):
    key_count = key_rows.shape[0]
    height = allowed.shape[0]
    factor = key_rows.shape[1] ** -0.5
    scores = (times_transposed(flat_queries, key_rows) * factor).reshape(height, group_size, key_count)
    window = jnp.concatenate([jnp.ones((height, key_count - allowed.shape[1]), dtype=jnp.bool_), allowed], axis=1)
    scores = jnp.where(window[:, None, :], scores, MASKED)
    highest = jnp.max(scores, axis=2, keepdims=True)
    powers = jnp.exp(scores - highest)
    totals = jnp.sum(powers, axis=2, keepdims=True)
    return (powers / totals).reshape(height * group_size, key_count)


def block_terms(q_block, cot_block, key_rows, value_rows, allowed):
    height = q_block.shape[0]
    group_size = HEADS // KV_HEADS
    span_cols = group_size * HEAD_DIM
    factor = HEAD_DIM ** -0.5
    outputs, q_grads, key_terms, value_terms = [], [], [], []
    for kv_index in range(KV_HEADS):
        flat_queries = q_block[:, kv_index * span_cols:(kv_index + 1) * span_cols].reshape(height * group_size, HEAD_DIM)
        flat_cot = cot_block[:, kv_index * span_cols:(kv_index + 1) * span_cols].reshape(height * group_size, HEAD_DIM)
        key_slice = key_rows[:, kv_index * HEAD_DIM:(kv_index + 1) * HEAD_DIM]
        value_slice = value_rows[:, kv_index * HEAD_DIM:(kv_index + 1) * HEAD_DIM]
        chances = probabilities(flat_queries, key_slice, allowed, group_size)
        rounded = chances.astype(jnp.bfloat16)
        attended = jnp.dot(rounded, value_slice, preferred_element_type=jnp.float32).astype(jnp.bfloat16)
        row_delta = jnp.sum(flat_cot.astype(jnp.float32) * attended.astype(jnp.float32), axis=1, keepdims=True)
        slopes = times_transposed(flat_cot, value_slice)
        score_grad = (chances * (slopes - row_delta)).astype(jnp.bfloat16)
        q_part = (jnp.dot(score_grad, key_slice, preferred_element_type=jnp.float32) * factor).astype(jnp.bfloat16)
        outputs.append(attended.reshape(height, span_cols))
        q_grads.append(q_part.reshape(height, span_cols))
        key_terms.append(transposed_times(score_grad, flat_queries) * factor)
        value_terms.append(transposed_times(rounded, flat_cot))
    return (jnp.concatenate(outputs, axis=1), jnp.concatenate(q_grads, axis=1),
            jnp.concatenate(key_terms, axis=1), jnp.concatenate(value_terms, axis=1))


def reference(queries, answer_keys, answer_values, prompt_keys, prompt_values, out_grad, weights, lengths):
    height = ROWS_DEV
    columns = KV_HEADS * HEAD_DIM
    cotangent = (weights[:, None] * out_grad.astype(jnp.float32)).astype(jnp.bfloat16)
    padding = jnp.zeros((2 * height, columns), jnp.bfloat16)
    padded_keys = jnp.concatenate([padding, answer_keys], axis=0)
    padded_values = jnp.concatenate([padding, answer_values], axis=0)
    own_offsets = jnp.arange(height, dtype=jnp.int32)
    key_offsets = jnp.arange(3 * height, dtype=jnp.int32)

    def advance(running, block_index):
        prompt_key_sum, prompt_value_sum, answer_key_sum, answer_value_sum = running
        start_row = block_index * height
        q_block = lax.dynamic_slice_in_dim(queries, start_row, height, 0)
        cot_block = lax.dynamic_slice_in_dim(cotangent, start_row, height, 0)
        window_keys = lax.dynamic_slice_in_dim(padded_keys, start_row, 3 * height, 0)
        window_values = lax.dynamic_slice_in_dim(padded_values, start_row, 3 * height, 0)
        own_pos = start_row + own_offsets
        key_pos = start_row - 2 * height + key_offsets
        own_seg = segment_of(own_pos, lengths)
        key_seg = segment_of(key_pos, lengths)
        allowed = (key_pos[None, :] >= 0) & (key_pos[None, :] <= own_pos[:, None]) & (key_seg[None, :] == own_seg[:, None])
        key_rows = jnp.concatenate([prompt_keys, window_keys], axis=0)
        value_rows = jnp.concatenate([prompt_values, window_values], axis=0)
        outputs, q_grads, key_terms, value_terms = block_terms(q_block, cot_block, key_rows, value_rows, allowed)
        prompt_key_sum = prompt_key_sum + key_terms[:PROMPT]
        prompt_value_sum = prompt_value_sum + value_terms[:PROMPT]
        answer_key_sum = lax.dynamic_update_slice_in_dim(
            answer_key_sum, lax.dynamic_slice_in_dim(answer_key_sum, start_row, 3 * height, 0) + key_terms[PROMPT:], start_row, 0)
        answer_value_sum = lax.dynamic_update_slice_in_dim(
            answer_value_sum, lax.dynamic_slice_in_dim(answer_value_sum, start_row, 3 * height, 0) + value_terms[PROMPT:], start_row, 0)
        return (prompt_key_sum, prompt_value_sum, answer_key_sum, answer_value_sum), (outputs, q_grads)

    initial = (jnp.zeros((PROMPT, columns), jnp.float32), jnp.zeros((PROMPT, columns), jnp.float32),
               jnp.zeros((ROWS + 2 * height, columns), jnp.float32), jnp.zeros((ROWS + 2 * height, columns), jnp.float32))
    running, stacked = lax.scan(advance, initial, jnp.arange(N_ROW, dtype=jnp.int32))
    attn_out = stacked[0].reshape(ROWS, HEADS * HEAD_DIM)
    q_grad = stacked[1].reshape(ROWS, HEADS * HEAD_DIM)
    answer_key_grad = running[2][2 * height:].astype(jnp.bfloat16)
    answer_value_grad = running[3][2 * height:].astype(jnp.bfloat16)
    return attn_out, q_grad, answer_key_grad, answer_value_grad, running[0], running[1]
```

```python
import functools
import math

import jax
import jax.numpy as jnp
from jax import lax
from jax.experimental import pallas as pl
from jax.experimental.pallas import tpu as pltpu
from jax.sharding import PartitionSpec as P

HEAD_DIM = 128
MASKED = -1e30
MESH = pl.DeviceIdType.MESH
NT = (((1,), (1,)), ((), ()))


def dot(a, b):
    return jnp.dot(a, b, preferred_element_type=jnp.float32)


def twice(x):
    return jnp.concatenate([x, x], axis=1)


def kernel(
    n, kv_heads, group,
    q_hbm, og_hbm, ak, av, pk, pv, w, lens,
    attn_hbm, dq_hbm, akg, avg, pkg, pvg,
    qv, ogv, attn_v, dq_v, win, pst, pgath, psend, precv, gsend, grecv, own,
    qs, cots, kcat, vcat, kt, vt, p_all, ds_all, bias, tri_b, wfull,
    in_sem, out_sem, st_sem, win_send, win_recv, pg_send, pg_recv,
    pr_send, pr_recv, gr_send, gr_recv,
):
    me = lax.axis_index("row")
    height = ak.shape[0]
    d = HEAD_DIM
    span = group * d
    prompt = pk.shape[0] * n
    factor = d ** (-0.5)
    log_factor = factor * math.log2(math.e)

    def peer(k):
        return lax.rem(me + k, n)

    def cols(g, width):
        return pl.ds(pl.multiple_of(g * width, width), width)

    def in_copies(g):
        return (
            pltpu.make_async_copy(q_hbm.at[:, cols(g, span)], qv.at[g], in_sem.at[g, 0]),
            pltpu.make_async_copy(og_hbm.at[:, cols(g, span)], ogv.at[g], in_sem.at[g, 1]),
        )

    def out_copies(g):
        return (
            pltpu.make_async_copy(attn_v.at[g], attn_hbm.at[:, cols(g, span)], out_sem.at[g, 0]),
            pltpu.make_async_copy(dq_v.at[g], dq_hbm.at[:, cols(g, span)], out_sem.at[g, 1]),
        )

    def stage_copies(g):
        return (
            pltpu.make_async_copy(pk.at[:, cols(g, d)], pst.at[g, 0], st_sem.at[g, 0]),
            pltpu.make_async_copy(pv.at[:, cols(g, d)], pst.at[g, 1], st_sem.at[g, 1]),
        )

    def win_copy(g, far, which):
        return pltpu.make_async_remote_copy(
            src_ref=(ak, av)[which].at[:, cols(g, d)],
            dst_ref=win.at[g, far, which],
            send_sem=win_send.at[g, far, which],
            recv_sem=win_recv.at[g, far, which],
            device_id={"row": peer(1 + far)},
            device_id_type=MESH,
        )

    def gather_copy(g, k):
        return pltpu.make_async_remote_copy(
            src_ref=pst.at[g],
            dst_ref=pgath.at[g, me],
            send_sem=pg_send.at[g],
            recv_sem=pg_recv.at[g],
            device_id={"row": peer(k)},
            device_id_type=MESH,
        )

    def reduce_copy(g, k):
        return pltpu.make_async_remote_copy(
            src_ref=psend.at[g, peer(k)],
            dst_ref=precv.at[g, me],
            send_sem=pr_send.at[g],
            recv_sem=pr_recv.at[g],
            device_id={"row": peer(k)},
            device_id_type=MESH,
        )

    def back_copy(g, far):
        return pltpu.make_async_remote_copy(
            src_ref=gsend.at[g, far],
            dst_ref=grecv.at[g, far],
            send_sem=gr_send.at[g, far],
            recv_sem=gr_recv.at[g, far],
            device_id={"row": peer(n - 1 - far)},
            device_id_type=MESH,
        )

    barrier = pltpu.get_barrier_semaphore()

    @pl.loop(1, n)
    def _(k):
        pl.semaphore_signal(barrier, inc=1, device_id={"row": peer(k)}, device_id_type=MESH)

    for g in range(kv_heads):
        for copy in stage_copies(g):
            copy.start()
    for g in range(kv_heads):
        for copy in in_copies(g):
            copy.start()

    answers = lens.shape[1]
    row = lax.broadcasted_iota(jnp.int32, (answers, answers), 0)
    col = lax.broadcasted_iota(jnp.int32, (answers, answers), 1)
    starts = jnp.sum(
        jnp.where(col < row, jnp.broadcast_to(lens[...], (answers, answers)), 0),
        axis=1, keepdims=True,
    )
    pos = me * height + lax.broadcasted_iota(jnp.int32, (1, height), 1)
    first = jnp.max(jnp.where(starts <= pos, starts, 0), axis=0, keepdims=True)
    key = lax.broadcasted_iota(jnp.int32, (height, height), 0)
    query = lax.broadcasted_iota(jnp.int32, (height, height), 1)
    tri = key <= query
    base = me * height
    near = jnp.where(key + (base - height) >= first, 0.0, MASKED)
    both = jnp.where(tri, key + base, key + (base - 2 * height))
    both = jnp.where(both >= first, 0.0, MASKED)
    bias[0] = near
    bias[1] = both
    tri_b[...] = tri.astype(jnp.float32).astype(jnp.bfloat16)
    wfull[...] = jnp.broadcast_to(w[...], (height, height)).T

    for g in range(kv_heads):
        for copy in stage_copies(g):
            copy.wait()
    pl.semaphore_wait(barrier, n - 1)

    @pl.loop(0, kv_heads)
    def _(g):
        pltpu.make_async_copy(pst.at[g], pgath.at[g, me], pg_recv.at[g]).start()

        @pl.loop(1, n)
        def _(k):
            gather_copy(g, k).start()

        for far in range(2):
            for which in range(2):
                win_copy(g, far, which).start()

    @pl.loop(0, kv_heads)
    def _(g):
        for copy in in_copies(g):
            copy.wait()
        for h in range(group):
            lanes = slice(h * d, (h + 1) * d)
            rows = slice(h * height, (h + 1) * height)
            qs[rows, :] = qv[g, :, lanes]
            cots[rows, :] = (wfull[...] * ogv[g, :, lanes].astype(jnp.float32)).astype(jnp.bfloat16)
        pltpu.make_async_copy(pgath.at[g], pgath.at[g], pg_recv.at[g]).wait()
        for far in range(2):
            for which in range(2):
                win_copy(g, far, which).wait_recv()
        at1, at2, at3 = prompt, prompt + height, prompt + 2 * height
        for which, (cat, tr, mine) in enumerate(((kcat, kt, ak), (vcat, vt, av))):
            gathered = pgath[g, :, which].astype(jnp.float32).reshape(prompt, d)
            cat[:at1, :] = gathered.astype(jnp.bfloat16)
            cat[at1:at2, :] = win[g, 0, which]
            cat[at2:at3, :] = win[g, 1, which]
            cat[at3:, :] = mine[:, cols(g, d)]
            tr[...] = cat[...].T
        tri2 = twice(tri)
        for pair in range(group // 2):
            rows = slice(pair * 2 * height, (pair + 1) * 2 * height)
            s = lax.dot_general(kcat[...], qs[rows, :], NT, preferred_element_type=jnp.float32)
            s_p = s[:at1]
            s_1 = s[at1:at2] + twice(bias[0])
            s_c = jnp.where(tri2, s[at3:], s[at2:at3]) + twice(bias[1])
            top = jnp.maximum(
                jnp.maximum(jnp.max(s_p, axis=0, keepdims=True), jnp.max(s_1, axis=0, keepdims=True)),
                jnp.max(s_c, axis=0, keepdims=True),
            )
            e_p = jnp.exp2((s_p - top) * log_factor)
            e_1 = jnp.exp2((s_1 - top) * log_factor)
            e_c = jnp.exp2((s_c - top) * log_factor)
            total = (
                jnp.sum(e_p, axis=0, keepdims=True)
                + jnp.sum(e_1, axis=0, keepdims=True)
                + jnp.sum(e_c, axis=0, keepdims=True)
            )
            inv = 1.0 / total
            c_p, c_1, c_c = e_p * inv, e_1 * inv, e_c * inv
            trib2 = twice(tri_b[...])
            p_all[:at1, rows] = c_p.astype(jnp.bfloat16)
            p_all[at1:at2, rows] = c_1.astype(jnp.bfloat16)
            b_c = c_c.astype(jnp.bfloat16)
            b_d = b_c * trib2
            p_all[at2:at3, rows] = b_c - b_d
            p_all[at3:, rows] = b_d
            out_t = dot(vt[...], p_all[:, rows]).astype(jnp.bfloat16)
            cot_t = cots[rows, :].T
            delta = jnp.sum(
                cot_t.astype(jnp.float32) * out_t.astype(jnp.float32), axis=0, keepdims=True
            )
            slopes = dot(vcat[...], cot_t)
            ds_all[:at1, rows] = (c_p * (slopes[:at1] - delta)).astype(jnp.bfloat16)
            ds_all[at1:at2, rows] = (c_1 * (slopes[at1:at2] - delta)).astype(jnp.bfloat16)
            s_c = jnp.where(tri2, slopes[at3:], slopes[at2:at3])
            g_c = (c_c * (s_c - delta)).astype(jnp.bfloat16)
            g_d = g_c * trib2
            ds_all[at2:at3, rows] = g_c - g_d
            ds_all[at3:, rows] = g_d
            dq_t = (dot(kt[...], ds_all[:, rows]) * factor).astype(jnp.bfloat16)
            out, dq = out_t.T, dq_t.T
            for j in range(2):
                lanes = slice((2 * pair + j) * d, (2 * pair + j + 1) * d)
                attn_v[g, :, lanes] = out[j * height : (j + 1) * height]
                dq_v[g, :, lanes] = dq[j * height : (j + 1) * height]
        for copy in out_copies(g):
            copy.start()
        for which in range(2):
            if which == 0:
                part = dot(ds_all[...], qs[...]) * factor
            else:
                part = dot(p_all[...], cots[...])
            psend[g, :, which] = part[:at1].reshape(n, prompt // n, d).astype(jnp.bfloat16)
            gsend[g, 0, which] = part[at1:at2].astype(jnp.bfloat16)
            gsend[g, 1, which] = part[at2:at3].astype(jnp.bfloat16)
            own[g, which] = part[at3:]
        back_copy(g, 1).start()
        back_copy(g, 0).start()
        pltpu.make_async_copy(psend.at[g, me], precv.at[g, me], pr_recv.at[g]).start()

        @pl.loop(1, n)
        def _(k):
            reduce_copy(g, k).start()

    for g in range(kv_heads):
        lanes = slice(g * d, (g + 1) * d)
        for far in range(2):
            back_copy(g, far).wait_recv()
        for which, grad in enumerate((akg, avg)):
            grad[:, lanes] = (
                own[g, which]
                + grecv[g, 0, which].astype(jnp.float32)
                + grecv[g, 1, which].astype(jnp.float32)
            ).astype(jnp.bfloat16)
        pltpu.make_async_copy(precv.at[g], precv.at[g], pr_recv.at[g]).wait()
        for which, grad in enumerate((pkg, pvg)):
            grad[:, lanes] = jnp.sum(precv[g, :, which].astype(jnp.float32), axis=0)

    for g in range(kv_heads):
        for copy in out_copies(g):
            copy.wait()
        for far in range(2):
            back_copy(g, far).wait_send()
            for which in range(2):
                win_copy(g, far, which).wait_send()
        sent = pgath.at[g, pl.ds(0, n - 1)]
        pltpu.make_async_copy(sent, sent, pg_send.at[g]).wait()
        sent = precv.at[g, pl.ds(0, n - 1)]
        pltpu.make_async_copy(sent, sent, pr_send.at[g]).wait()


def per_device(n, queries, answer_keys, answer_values, prompt_keys, prompt_values, out_grad, weights, lengths):
    height = queries.shape[0]
    d = HEAD_DIM
    columns = answer_keys.shape[1]
    kv_heads = columns // d
    group = queries.shape[1] // columns
    own_prompt = prompt_keys.shape[0]
    keys = own_prompt * n + 3 * height
    span = group * d
    bf16, f32 = jnp.bfloat16, jnp.float32
    vmem = pl.BlockSpec(memory_space=pltpu.VMEM)
    hbm = pl.BlockSpec(memory_space=pl.ANY)
    dma = pltpu.SemaphoreType.DMA
    return pl.pallas_call(
        functools.partial(kernel, n, kv_heads, group),
        out_shape=(
            jax.ShapeDtypeStruct(queries.shape, bf16),
            jax.ShapeDtypeStruct(queries.shape, bf16),
            jax.ShapeDtypeStruct(answer_keys.shape, bf16),
            jax.ShapeDtypeStruct(answer_keys.shape, bf16),
            jax.ShapeDtypeStruct(prompt_keys.shape, f32),
            jax.ShapeDtypeStruct(prompt_keys.shape, f32),
        ),
        in_specs=[hbm, hbm] + [vmem] * 6,
        out_specs=(hbm, hbm) + (vmem,) * 4,
        scratch_shapes=[
            pltpu.VMEM((kv_heads, height, span), bf16),
            pltpu.VMEM((kv_heads, height, span), bf16),
            pltpu.VMEM((kv_heads, height, span), bf16),
            pltpu.VMEM((kv_heads, height, span), bf16),
            pltpu.VMEM((kv_heads, 2, 2, height, d), bf16),
            pltpu.VMEM((kv_heads, 2, own_prompt, d), bf16),
            pltpu.VMEM((kv_heads, n, 2, own_prompt, d), bf16),
            pltpu.VMEM((kv_heads, n, 2, own_prompt, d), bf16),
            pltpu.VMEM((kv_heads, n, 2, own_prompt, d), bf16),
            pltpu.VMEM((kv_heads, 2, 2, height, d), bf16),
            pltpu.VMEM((kv_heads, 2, 2, height, d), bf16),
            pltpu.VMEM((kv_heads, 2, height, d), f32),
            pltpu.VMEM((group * height, d), bf16),
            pltpu.VMEM((group * height, d), bf16),
            pltpu.VMEM((keys, d), bf16),
            pltpu.VMEM((keys, d), bf16),
            pltpu.VMEM((d, keys), bf16),
            pltpu.VMEM((d, keys), bf16),
            pltpu.VMEM((keys, group * height), bf16),
            pltpu.VMEM((keys, group * height), bf16),
            pltpu.VMEM((2, height, height), f32),
            pltpu.VMEM((height, height), bf16),
            pltpu.VMEM((height, height), f32),
            dma((kv_heads, 2)),
            dma((kv_heads, 2)),
            dma((kv_heads, 2)),
            dma((kv_heads, 2, 2)),
            dma((kv_heads, 2, 2)),
            dma((kv_heads,)),
            dma((kv_heads,)),
            dma((kv_heads,)),
            dma((kv_heads,)),
            dma((kv_heads, 2)),
            dma((kv_heads, 2)),
        ],
        compiler_params=pltpu.CompilerParams(
            collective_id=0, has_side_effects=True, vmem_limit_bytes=60 * 1024 * 1024
        ),
    )(
        queries, out_grad, answer_keys, answer_values, prompt_keys, prompt_values,
        weights.reshape(1, height), lengths.reshape(1, lengths.shape[0]),
    )


def solution(mesh):
    both = ("grp", "row")
    wide = P(both, None)
    return jax.shard_map(
        functools.partial(per_device, mesh.shape["row"]),
        mesh=mesh,
        in_specs=(wide,) * 6 + (P(both), P("grp")),
        out_specs=(wide,) * 6,
        check_vma=False,
    )
```

```python
import functools
import math

import jax
import jax.numpy as jnp
from jax import lax
from jax.experimental import pallas as pl
from jax.experimental.pallas import tpu as pltpu
from jax.sharding import PartitionSpec as P

HEAD_DIM = 128
MASKED = -1e30
MESH = pl.DeviceIdType.MESH
NT = (((1,), (1,)), ((), ()))


def dot(a, b):
    return jnp.dot(a, b, preferred_element_type=jnp.float32)


def twice(x):
    return jnp.concatenate([x, x], axis=1)


def kernel(
    n, kv_heads, group,
    q_hbm, og_hbm, ak, av, pk, pv, w, lens,
    attn_hbm, dq_hbm, akg, avg, pkg, pvg,
    qv, ogv, attn_v, dq_v, win, pst, pgath, psend, pmid, pred, precv,
    gsend, gmid, gout, grecv, own,
    qs, cots, kcat, vcat, kt, vt, p_all, ds_all, bias, tri_b, wfull,
    in_sem, out_sem, st_sem, win_send, win_recv, wr_send, pg_send, pg_recv, pp_send, pp_recv,
    pm_send, pm_recv, pr_send, pr_recv, gm_send, gm_recv, gr_send, gr_recv,
):
    me = lax.axis_index("row")
    height = ak.shape[0]
    d = HEAD_DIM
    span = group * d
    prompt = pk.shape[0] * n
    factor = d ** (-0.5)
    log_factor = factor * math.log2(math.e)

    chips = n // 2
    core = lax.rem(me, 2)
    chip = me // 2
    sibling = me + 1 - 2 * core
    across = lax.rem(me + n - 1 + 2 * core, n)

    def same(k):
        return lax.rem(me + 2 * k, n)

    def remote(src, dst, send, recv, target):
        return pltpu.make_async_remote_copy(
            src_ref=src, dst_ref=dst, send_sem=send, recv_sem=recv,
            device_id={"row": target}, device_id_type=MESH,
        )

    def cols(g, width):
        return pl.ds(pl.multiple_of(g * width, width), width)

    def in_copies(g):
        return (
            pltpu.make_async_copy(q_hbm.at[:, cols(g, span)], qv.at[g], in_sem.at[g, 0]),
            pltpu.make_async_copy(og_hbm.at[:, cols(g, span)], ogv.at[g], in_sem.at[g, 1]),
        )

    def out_copies(g):
        return (
            pltpu.make_async_copy(attn_v.at[g], attn_hbm.at[:, cols(g, span)], out_sem.at[g, 0]),
            pltpu.make_async_copy(dq_v.at[g], dq_hbm.at[:, cols(g, span)], out_sem.at[g, 1]),
        )

    def stage_copies(g):
        return (
            pltpu.make_async_copy(pk.at[:, cols(g, d)], pst.at[g, 0], st_sem.at[g, 0]),
            pltpu.make_async_copy(pv.at[:, cols(g, d)], pst.at[g, 1], st_sem.at[g, 1]),
        )

    def win_copy(g, far, which):
        return remote(
            (ak, av)[which].at[:, cols(g, d)], win.at[g, far, which],
            win_send.at[g, far, which], win_recv.at[g, far, which],
            same(1) if far else lax.rem(me + 1, n),
        )

    def win_relay(g, which):
        return remote(
            win.at[g, 0, which], win.at[g, 1, which],
            wr_send.at[g, which], win_recv.at[g, 1, which], sibling,
        )

    def gather_copy(g, k):
        return remote(
            pst.at[g], pgath.at[g, core, chip], pg_send.at[g], pg_recv.at[g], same(k)
        )

    def gather_relay(g):
        return remote(
            pgath.at[g, core], pgath.at[g, core], pp_send.at[g], pp_recv.at[g], sibling
        )

    def pair_copy(g):
        return remote(psend.at[g, 1 - core], pmid.at[g], pm_send.at[g], pm_recv.at[g], sibling)

    def reduce_copy(g, k):
        return remote(
            pred.at[g, lax.rem(chip + k, chips)], precv.at[g, chip],
            pr_send.at[g], pr_recv.at[g], same(k),
        )

    def mid_copy(g):
        return remote(gsend.at[g], gmid.at[g], gm_send.at[g], gm_recv.at[g], sibling)

    def back_copy(g, far):
        return remote(
            gsend.at[g, 1] if far else gout.at[g], grecv.at[g],
            gr_send.at[g, far], gr_recv.at[g], same(chips - 1) if far else across,
        )

    def relay(g):
        for which in range(2):
            win_copy(g, 0, which).wait_recv()

        @pl.when(core == 0)
        def _():
            for which in range(2):
                win_relay(g, which).start()

        here = pgath.at[g, core]
        pltpu.make_async_copy(here, here, pg_recv.at[g]).wait()
        gather_relay(g).start()

    def pass_on(g):
        pair_copy(g).wait_recv()
        pred[g] = (psend[g, core] + pmid[g]).astype(jnp.bfloat16)

        @pl.when(core == 0)
        def _():
            mid_copy(g).wait_recv()
            gout[g] = (
                gsend[g, 0].astype(jnp.float32) + gmid[g, 1].astype(jnp.float32)
            ).astype(jnp.bfloat16)
            own[g] = own[g] + gmid[g, 0].astype(jnp.float32)
            back_copy(g, 0).start()
            back_copy(g, 1).start()

        pltpu.make_async_copy(pred.at[g, chip], precv.at[g, chip], pr_recv.at[g]).start()

        @pl.loop(1, chips)
        def _(k):
            reduce_copy(g, k).start()

    barrier = pltpu.get_barrier_semaphore()

    @pl.loop(1, chips)
    def _(k):
        pl.semaphore_signal(barrier, inc=1, device_id={"row": same(k)}, device_id_type=MESH)

    for target in (sibling, across):
        pl.semaphore_signal(barrier, inc=1, device_id={"row": target}, device_id_type=MESH)

    for g in range(kv_heads):
        for copy in stage_copies(g):
            copy.start()
    for g in range(kv_heads):
        for copy in in_copies(g):
            copy.start()

    answers = lens.shape[1]
    row = lax.broadcasted_iota(jnp.int32, (answers, answers), 0)
    col = lax.broadcasted_iota(jnp.int32, (answers, answers), 1)
    starts = jnp.sum(
        jnp.where(col < row, jnp.broadcast_to(lens[...], (answers, answers)), 0),
        axis=1, keepdims=True,
    )
    pos = me * height + lax.broadcasted_iota(jnp.int32, (1, height), 1)
    first = jnp.max(jnp.where(starts <= pos, starts, 0), axis=0, keepdims=True)
    key = lax.broadcasted_iota(jnp.int32, (height, height), 0)
    query = lax.broadcasted_iota(jnp.int32, (height, height), 1)
    tri = key <= query
    base = me * height
    near = jnp.where(key + (base - height) >= first, 0.0, MASKED)
    both = jnp.where(tri, key + base, key + (base - 2 * height))
    both = jnp.where(both >= first, 0.0, MASKED)
    bias[0] = near
    bias[1] = both
    tri_b[...] = tri.astype(jnp.float32).astype(jnp.bfloat16)
    wfull[...] = jnp.broadcast_to(w[...], (height, height)).T

    for g in range(kv_heads):
        for copy in stage_copies(g):
            copy.wait()
    pl.semaphore_wait(barrier, chips + 1)

    @pl.loop(0, kv_heads)
    def _(g):
        pltpu.make_async_copy(pst.at[g], pgath.at[g, core, chip], pg_recv.at[g]).start()

        @pl.loop(1, chips)
        def _(k):
            gather_copy(g, k).start()

        for which in range(2):
            win_copy(g, 0, which).start()

        @pl.when(core == 0)
        def _():
            for which in range(2):
                win_copy(g, 1, which).start()

    @pl.loop(0, kv_heads)
    def _(g):
        @pl.when(g == 0)
        def _():
            relay(0)

        for copy in in_copies(g):
            copy.wait()
        for h in range(group):
            lanes = slice(h * d, (h + 1) * d)
            rows = slice(h * height, (h + 1) * height)
            qs[rows, :] = qv[g, :, lanes]
            cots[rows, :] = (wfull[...] * ogv[g, :, lanes].astype(jnp.float32)).astype(jnp.bfloat16)
        there = pgath.at[g, 1 - core]
        pltpu.make_async_copy(there, there, pp_recv.at[g]).wait()
        for which in range(2):
            win_copy(g, 1, which).wait_recv()
        at1, at2, at3 = prompt, prompt + height, prompt + 2 * height
        for which, (cat, tr, mine) in enumerate(((kcat, kt, ak), (vcat, vt, av))):
            gathered = pgath[g, :, :, which].astype(jnp.float32).reshape(prompt, d)
            cat[:at1, :] = gathered.astype(jnp.bfloat16)
            cat[at1:at2, :] = win[g, 0, which]
            cat[at2:at3, :] = win[g, 1, which]
            cat[at3:, :] = mine[:, cols(g, d)]
            tr[...] = cat[...].T
        tri2 = twice(tri)
        for pair in range(group // 2):
            if pair == group // 4:
                @pl.when(g > 0)
                def _():
                    pass_on(g - 1)

                @pl.when(g < kv_heads - 1)
                def _():
                    relay(g + 1)

            rows = slice(pair * 2 * height, (pair + 1) * 2 * height)
            s = lax.dot_general(kcat[...], qs[rows, :], NT, preferred_element_type=jnp.float32)
            s_p = s[:at1]
            s_1 = s[at1:at2] + twice(bias[0])
            s_c = jnp.where(tri2, s[at3:], s[at2:at3]) + twice(bias[1])
            top = jnp.maximum(
                jnp.maximum(jnp.max(s_p, axis=0, keepdims=True), jnp.max(s_1, axis=0, keepdims=True)),
                jnp.max(s_c, axis=0, keepdims=True),
            )
            e_p = jnp.exp2((s_p - top) * log_factor)
            e_1 = jnp.exp2((s_1 - top) * log_factor)
            e_c = jnp.exp2((s_c - top) * log_factor)
            total = (
                jnp.sum(e_p, axis=0, keepdims=True)
                + jnp.sum(e_1, axis=0, keepdims=True)
                + jnp.sum(e_c, axis=0, keepdims=True)
            )
            inv = 1.0 / total
            c_p, c_1, c_c = e_p * inv, e_1 * inv, e_c * inv
            trib2 = twice(tri_b[...])
            p_all[:at1, rows] = c_p.astype(jnp.bfloat16)
            p_all[at1:at2, rows] = c_1.astype(jnp.bfloat16)
            b_c = c_c.astype(jnp.bfloat16)
            b_d = b_c * trib2
            p_all[at2:at3, rows] = b_c - b_d
            p_all[at3:, rows] = b_d
            out_t = dot(vt[...], p_all[:, rows]).astype(jnp.bfloat16)
            cot_t = cots[rows, :].T
            delta = jnp.sum(
                cot_t.astype(jnp.float32) * out_t.astype(jnp.float32), axis=0, keepdims=True
            )
            slopes = dot(vcat[...], cot_t)
            ds_all[:at1, rows] = (c_p * (slopes[:at1] - delta)).astype(jnp.bfloat16)
            ds_all[at1:at2, rows] = (c_1 * (slopes[at1:at2] - delta)).astype(jnp.bfloat16)
            s_c = jnp.where(tri2, slopes[at3:], slopes[at2:at3])
            g_c = (c_c * (s_c - delta)).astype(jnp.bfloat16)
            g_d = g_c * trib2
            ds_all[at2:at3, rows] = g_c - g_d
            ds_all[at3:, rows] = g_d
            dq_t = (dot(kt[...], ds_all[:, rows]) * factor).astype(jnp.bfloat16)
            out, dq = out_t.T, dq_t.T
            for j in range(2):
                lanes = slice((2 * pair + j) * d, (2 * pair + j + 1) * d)
                attn_v[g, :, lanes] = out[j * height : (j + 1) * height]
                dq_v[g, :, lanes] = dq[j * height : (j + 1) * height]
        for copy in out_copies(g):
            copy.start()
        for which in range(2):
            if which == 0:
                part = dot(ds_all[...], qs[...]) * factor
            else:
                part = dot(p_all[...], cots[...])
            psend[g, :, :, which] = part[:at1].reshape(2, chips, prompt // n, d)
            gsend[g, 0, which] = part[at1:at2].astype(jnp.bfloat16)
            gsend[g, 1, which] = part[at2:at3].astype(jnp.bfloat16)
            own[g, which] = part[at3:]
        pair_copy(g).start()

        @pl.when(core == 1)
        def _():
            mid_copy(g).start()

    pass_on(kv_heads - 1)
    for g in range(kv_heads):
        lanes = slice(g * d, (g + 1) * d)
        back_copy(g, 0).wait_recv()
        for which, grad in enumerate((akg, avg)):
            grad[:, lanes] = (own[g, which] + grecv[g, which].astype(jnp.float32)).astype(
                jnp.bfloat16
            )
        pltpu.make_async_copy(precv.at[g], precv.at[g], pr_recv.at[g]).wait()
        for which, grad in enumerate((pkg, pvg)):
            grad[:, lanes] = jnp.sum(precv[g, :, which].astype(jnp.float32), axis=0)

    for g in range(kv_heads):
        for copy in out_copies(g):
            copy.wait()
        pair_copy(g).wait_send()
        gather_relay(g).wait_send()
        for which in range(2):
            win_copy(g, 0, which).wait_send()
        sent = pgath.at[g, 0, pl.ds(0, chips - 1)]
        pltpu.make_async_copy(sent, sent, pg_send.at[g]).wait()
        sent = precv.at[g, pl.ds(0, chips - 1)]
        pltpu.make_async_copy(sent, sent, pr_send.at[g]).wait()

        @pl.when(core == 0)
        def _():
            for which in range(2):
                win_copy(g, 1, which).wait_send()
                win_relay(g, which).wait_send()
                back_copy(g, which).wait_send()

        @pl.when(core == 1)
        def _():
            mid_copy(g).wait_send()


def per_device(n, queries, answer_keys, answer_values, prompt_keys, prompt_values, out_grad, weights, lengths):
    height = queries.shape[0]
    d = HEAD_DIM
    columns = answer_keys.shape[1]
    kv_heads = columns // d
    group = queries.shape[1] // columns
    own_prompt = prompt_keys.shape[0]
    keys = own_prompt * n + 3 * height
    span = group * d
    bf16, f32 = jnp.bfloat16, jnp.float32
    vmem = pl.BlockSpec(memory_space=pltpu.VMEM)
    hbm = pl.BlockSpec(memory_space=pl.ANY)
    dma = pltpu.SemaphoreType.DMA
    return pl.pallas_call(
        functools.partial(kernel, n, kv_heads, group),
        out_shape=(
            jax.ShapeDtypeStruct(queries.shape, bf16),
            jax.ShapeDtypeStruct(queries.shape, bf16),
            jax.ShapeDtypeStruct(answer_keys.shape, bf16),
            jax.ShapeDtypeStruct(answer_keys.shape, bf16),
            jax.ShapeDtypeStruct(prompt_keys.shape, f32),
            jax.ShapeDtypeStruct(prompt_keys.shape, f32),
        ),
        in_specs=[hbm, hbm] + [vmem] * 6,
        out_specs=(hbm, hbm) + (vmem,) * 4,
        scratch_shapes=[
            pltpu.VMEM((kv_heads, height, span), bf16),
            pltpu.VMEM((kv_heads, height, span), bf16),
            pltpu.VMEM((kv_heads, height, span), bf16),
            pltpu.VMEM((kv_heads, height, span), bf16),
            pltpu.VMEM((kv_heads, 2, 2, height, d), bf16),
            pltpu.VMEM((kv_heads, 2, own_prompt, d), bf16),
            pltpu.VMEM((kv_heads, 2, n // 2, 2, own_prompt, d), bf16),
            pltpu.VMEM((kv_heads, 2, n // 2, 2, own_prompt, d), f32),
            pltpu.VMEM((kv_heads, n // 2, 2, own_prompt, d), f32),
            pltpu.VMEM((kv_heads, n // 2, 2, own_prompt, d), bf16),
            pltpu.VMEM((kv_heads, n // 2, 2, own_prompt, d), bf16),
            pltpu.VMEM((kv_heads, 2, 2, height, d), bf16),
            pltpu.VMEM((kv_heads, 2, 2, height, d), bf16),
            pltpu.VMEM((kv_heads, 2, height, d), bf16),
            pltpu.VMEM((kv_heads, 2, height, d), bf16),
            pltpu.VMEM((kv_heads, 2, height, d), f32),
            pltpu.VMEM((group * height, d), bf16),
            pltpu.VMEM((group * height, d), bf16),
            pltpu.VMEM((keys, d), bf16),
            pltpu.VMEM((keys, d), bf16),
            pltpu.VMEM((d, keys), bf16),
            pltpu.VMEM((d, keys), bf16),
            pltpu.VMEM((keys, group * height), bf16),
            pltpu.VMEM((keys, group * height), bf16),
            pltpu.VMEM((2, height, height), f32),
            pltpu.VMEM((height, height), bf16),
            pltpu.VMEM((height, height), f32),
            dma((kv_heads, 2)),
            dma((kv_heads, 2)),
            dma((kv_heads, 2)),
            dma((kv_heads, 2, 2)),
            dma((kv_heads, 2, 2)),
            dma((kv_heads, 2)),
            *[dma((kv_heads,))] * 10,
            dma((kv_heads, 2)),
            dma((kv_heads,)),
        ],
        compiler_params=pltpu.CompilerParams(
            collective_id=0, has_side_effects=True, vmem_limit_bytes=60 * 1024 * 1024
        ),
    )(
        queries, out_grad, answer_keys, answer_values, prompt_keys, prompt_values,
        weights.reshape(1, height), lengths.reshape(1, lengths.shape[0]),
    )


def solution(mesh):
    both = ("grp", "row")
    wide = P(both, None)
    return jax.shard_map(
        functools.partial(per_device, mesh.shape["row"]),
        mesh=mesh,
        in_specs=(wide,) * 6 + (P(both), P("grp")),
        out_specs=(wide,) * 6,
        check_vma=False,
    )
```

```python
import functools
import math

import jax
import jax.numpy as jnp
from jax import lax
from jax.experimental import pallas as pl
from jax.experimental.pallas import tpu as pltpu
from jax.sharding import PartitionSpec as P

HEAD_DIM = 128
MASKED = -1e30
MESH = pl.DeviceIdType.MESH
NT = (((1,), (1,)), ((), ()))


def dot(a, b):
    return jnp.dot(a, b, preferred_element_type=jnp.float32)


def twice(x):
    return jnp.concatenate([x, x], axis=1)


def kernel(
    n, kv_heads, group,
    q_hbm, og_hbm, ak, av, pk, pv, w, lens,
    attn_v, dq_v, akg, avg, pkg, pvg,
    qv, ogv, win, pst, pgath, psend, pmid, pred, precv,
    gsend, gmid, gout, grecv, own,
    qs, cots, kcat, vcat, kt, vt, p_all, ds_all, bias, tri_b, wfull,
    in_sem, st_sem, win_send, win_recv, wr_send, pg_send, pg_recv, pp_send, pp_recv,
    pm_send, pm_recv, pr_send, pr_recv, gm_send, gm_recv, gr_send, gr_recv,
):
    me = lax.axis_index("row")
    height = ak.shape[0]
    d = HEAD_DIM
    span = group * d
    prompt = pk.shape[0] * n
    factor = d ** (-0.5)
    log_factor = factor * math.log2(math.e)

    chips = n // 2
    core = lax.rem(me, 2)
    chip = me // 2
    sibling = me + 1 - 2 * core
    across = lax.rem(me + n - 1 + 2 * core, n)

    def same(k):
        return lax.rem(me + 2 * k, n)

    def remote(src, dst, send, recv, target):
        return pltpu.make_async_remote_copy(
            src_ref=src, dst_ref=dst, send_sem=send, recv_sem=recv,
            device_id={"row": target}, device_id_type=MESH,
        )

    def cols(g, width):
        return pl.ds(pl.multiple_of(g * width, width), width)

    def in_copies(g):
        return (
            pltpu.make_async_copy(q_hbm.at[:, cols(g, span)], qv.at[g], in_sem.at[g, 0]),
            pltpu.make_async_copy(og_hbm.at[:, cols(g, span)], ogv.at[g], in_sem.at[g, 1]),
        )

    def stage_copies(g):
        return (
            pltpu.make_async_copy(pk.at[:, cols(g, d)], pst.at[g, 0], st_sem.at[g, 0]),
            pltpu.make_async_copy(pv.at[:, cols(g, d)], pst.at[g, 1], st_sem.at[g, 1]),
        )

    def win_copy(g, far, which):
        return remote(
            (ak, av)[which].at[:, cols(g, d)], win.at[g, far, which],
            win_send.at[g, far, which], win_recv.at[g, far, which],
            same(1) if far else lax.rem(me + 1, n),
        )

    def win_relay(g, which):
        return remote(
            win.at[g, 0, which], win.at[g, 1, which],
            wr_send.at[g, which], win_recv.at[g, 1, which], sibling,
        )

    def gather_copy(g, k):
        return remote(
            pst.at[g], pgath.at[g, core, chip], pg_send.at[g], pg_recv.at[g], same(k)
        )

    def gather_relay(g):
        return remote(
            pgath.at[g, core], pgath.at[g, core], pp_send.at[g], pp_recv.at[g], sibling
        )

    def pair_copy(g):
        return remote(psend.at[g, 1 - core], pmid.at[g], pm_send.at[g], pm_recv.at[g], sibling)

    def reduce_copy(g, k):
        return remote(
            pred.at[g, lax.rem(chip + k, chips)], precv.at[g, chip],
            pr_send.at[g], pr_recv.at[g], same(k),
        )

    def mid_copy(g):
        return remote(gsend.at[g], gmid.at[g], gm_send.at[g], gm_recv.at[g], sibling)

    def back_copy(g, far):
        return remote(
            gsend.at[g, 1] if far else gout.at[g], grecv.at[g],
            gr_send.at[g, far], gr_recv.at[g], same(chips - 1) if far else across,
        )

    def relay(g):
        for which in range(2):
            win_copy(g, 0, which).wait_recv()

        @pl.when(core == 0)
        def _():
            for which in range(2):
                win_relay(g, which).start()

        here = pgath.at[g, core]
        pltpu.make_async_copy(here, here, pg_recv.at[g]).wait()
        gather_relay(g).start()

    def pass_on(g):
        pair_copy(g).wait_recv()
        pred[g] = (psend[g, core] + pmid[g]).astype(jnp.bfloat16)

        @pl.when(core == 0)
        def _():
            mid_copy(g).wait_recv()
            gout[g] = (
                gsend[g, 0].astype(jnp.float32) + gmid[g, 1].astype(jnp.float32)
            ).astype(jnp.bfloat16)
            own[g] = own[g] + gmid[g, 0].astype(jnp.float32)
            back_copy(g, 0).start()
            back_copy(g, 1).start()

        pltpu.make_async_copy(pred.at[g, chip], precv.at[g, chip], pr_recv.at[g]).start()

        @pl.loop(1, chips)
        def _(k):
            reduce_copy(g, k).start()

    barrier = pltpu.get_barrier_semaphore()

    @pl.loop(1, chips)
    def _(k):
        pl.semaphore_signal(barrier, inc=1, device_id={"row": same(k)}, device_id_type=MESH)

    for target in (sibling, across):
        pl.semaphore_signal(barrier, inc=1, device_id={"row": target}, device_id_type=MESH)

    for g in range(kv_heads):
        for copy in stage_copies(g):
            copy.start()
    for g in range(kv_heads):
        for copy in in_copies(g):
            copy.start()

    answers = lens.shape[1]
    row = lax.broadcasted_iota(jnp.int32, (answers, answers), 0)
    col = lax.broadcasted_iota(jnp.int32, (answers, answers), 1)
    starts = jnp.sum(
        jnp.where(col < row, jnp.broadcast_to(lens[...], (answers, answers)), 0),
        axis=1, keepdims=True,
    )
    pos = me * height + lax.broadcasted_iota(jnp.int32, (1, height), 1)
    first = jnp.max(jnp.where(starts <= pos, starts, 0), axis=0, keepdims=True)
    key = lax.broadcasted_iota(jnp.int32, (height, height), 0)
    query = lax.broadcasted_iota(jnp.int32, (height, height), 1)
    tri = key <= query
    base = me * height
    near = jnp.where(key + (base - height) >= first, 0.0, MASKED)
    both = jnp.where(tri, key + base, key + (base - 2 * height))
    both = jnp.where(both >= first, 0.0, MASKED)
    bias[0] = near
    bias[1] = both
    tri_b[...] = tri.astype(jnp.float32).astype(jnp.bfloat16)
    wfull[...] = jnp.broadcast_to(w[...], (height, height)).T

    for g in range(kv_heads):
        for copy in stage_copies(g):
            copy.wait()
    pl.semaphore_wait(barrier, chips + 1)

    @pl.loop(0, kv_heads)
    def _(g):
        pltpu.make_async_copy(pst.at[g], pgath.at[g, core, chip], pg_recv.at[g]).start()

        @pl.loop(1, chips)
        def _(k):
            gather_copy(g, k).start()

        for which in range(2):
            win_copy(g, 0, which).start()

        @pl.when(core == 0)
        def _():
            for which in range(2):
                win_copy(g, 1, which).start()

    @pl.loop(0, kv_heads)
    def _(g):
        @pl.when(g == 0)
        def _():
            relay(0)

        for copy in in_copies(g):
            copy.wait()
        for h in range(group):
            lanes = slice(h * d, (h + 1) * d)
            rows = slice(h * height, (h + 1) * height)
            qs[rows, :] = qv[g, :, lanes]
            cots[rows, :] = (wfull[...] * ogv[g, :, lanes].astype(jnp.float32)).astype(jnp.bfloat16)
        there = pgath.at[g, 1 - core]
        pltpu.make_async_copy(there, there, pp_recv.at[g]).wait()
        for which in range(2):
            win_copy(g, 1, which).wait_recv()
        at1, at2, at3 = prompt, prompt + height, prompt + 2 * height
        for which, (cat, tr, mine) in enumerate(((kcat, kt, ak), (vcat, vt, av))):
            gathered = pgath[g, :, :, which].astype(jnp.float32).reshape(prompt, d)
            cat[:at1, :] = gathered.astype(jnp.bfloat16)
            cat[at1:at2, :] = win[g, 0, which]
            cat[at2:at3, :] = win[g, 1, which]
            cat[at3:, :] = mine[:, cols(g, d)]
            tr[...] = cat[...].T
        tri2 = twice(tri)
        for pair in range(group // 2):
            if pair == group // 4:
                @pl.when(g > 0)
                def _():
                    pass_on(g - 1)

                @pl.when(g < kv_heads - 1)
                def _():
                    relay(g + 1)

            rows = slice(pair * 2 * height, (pair + 1) * 2 * height)
            s = lax.dot_general(kcat[...], qs[rows, :], NT, preferred_element_type=jnp.float32)
            s_p = s[:at1]
            s_1 = s[at1:at2] + twice(bias[0])
            s_c = jnp.where(tri2, s[at3:], s[at2:at3]) + twice(bias[1])
            top = jnp.maximum(
                jnp.maximum(jnp.max(s_p, axis=0, keepdims=True), jnp.max(s_1, axis=0, keepdims=True)),
                jnp.max(s_c, axis=0, keepdims=True),
            )
            e_p = jnp.exp2((s_p - top) * log_factor)
            e_1 = jnp.exp2((s_1 - top) * log_factor)
            e_c = jnp.exp2((s_c - top) * log_factor)
            total = (
                jnp.sum(e_p, axis=0, keepdims=True)
                + jnp.sum(e_1, axis=0, keepdims=True)
                + jnp.sum(e_c, axis=0, keepdims=True)
            )
            inv = 1.0 / total
            c_p, c_1, c_c = e_p * inv, e_1 * inv, e_c * inv
            trib2 = twice(tri_b[...])
            p_all[:at1, rows] = c_p.astype(jnp.bfloat16)
            p_all[at1:at2, rows] = c_1.astype(jnp.bfloat16)
            b_c = c_c.astype(jnp.bfloat16)
            b_d = b_c * trib2
            p_all[at2:at3, rows] = b_c - b_d
            p_all[at3:, rows] = b_d
            out_t = dot(vt[...], p_all[:, rows]).astype(jnp.bfloat16)
            cot_t = cots[rows, :].T
            delta = jnp.sum(
                cot_t.astype(jnp.float32) * out_t.astype(jnp.float32), axis=0, keepdims=True
            )
            slopes = dot(vcat[...], cot_t)
            ds_all[:at1, rows] = (c_p * (slopes[:at1] - delta)).astype(jnp.bfloat16)
            ds_all[at1:at2, rows] = (c_1 * (slopes[at1:at2] - delta)).astype(jnp.bfloat16)
            s_c = jnp.where(tri2, slopes[at3:], slopes[at2:at3])
            g_c = (c_c * (s_c - delta)).astype(jnp.bfloat16)
            g_d = g_c * trib2
            ds_all[at2:at3, rows] = g_c - g_d
            ds_all[at3:, rows] = g_d
            dq_t = (dot(kt[...], ds_all[:, rows]) * factor).astype(jnp.bfloat16)
            out, dq = out_t.T, dq_t.T
            for j in range(2):
                lanes = slice((2 * pair + j) * d, (2 * pair + j + 1) * d)
                attn_v[g, :, lanes] = out[j * height : (j + 1) * height]
                dq_v[g, :, lanes] = dq[j * height : (j + 1) * height]
        for which in range(2):
            if which == 0:
                part = dot(ds_all[...], qs[...]) * factor
            else:
                part = dot(p_all[...], cots[...])
            psend[g, :, :, which] = part[:at1].reshape(2, chips, prompt // n, d)
            gsend[g, 0, which] = part[at1:at2].astype(jnp.bfloat16)
            gsend[g, 1, which] = part[at2:at3].astype(jnp.bfloat16)
            own[g, which] = part[at3:]
        pair_copy(g).start()

        @pl.when(core == 1)
        def _():
            mid_copy(g).start()

    pass_on(kv_heads - 1)
    for g in range(kv_heads):
        lanes = slice(g * d, (g + 1) * d)
        back_copy(g, 0).wait_recv()
        for which, grad in enumerate((akg, avg)):
            grad[:, lanes] = (own[g, which] + grecv[g, which].astype(jnp.float32)).astype(
                jnp.bfloat16
            )
        pltpu.make_async_copy(precv.at[g], precv.at[g], pr_recv.at[g]).wait()
        for which, grad in enumerate((pkg, pvg)):
            grad[:, lanes] = jnp.sum(precv[g, :, which].astype(jnp.float32), axis=0)

    for g in range(kv_heads):
        pair_copy(g).wait_send()
        gather_relay(g).wait_send()
        for which in range(2):
            win_copy(g, 0, which).wait_send()
        sent = pgath.at[g, 0, pl.ds(0, chips - 1)]
        pltpu.make_async_copy(sent, sent, pg_send.at[g]).wait()
        sent = precv.at[g, pl.ds(0, chips - 1)]
        pltpu.make_async_copy(sent, sent, pr_send.at[g]).wait()

        @pl.when(core == 0)
        def _():
            for which in range(2):
                win_copy(g, 1, which).wait_send()
                win_relay(g, which).wait_send()
                back_copy(g, which).wait_send()

        @pl.when(core == 1)
        def _():
            mid_copy(g).wait_send()


def write_out(kv_heads, span, attn_v, dq_v, akg, avg, pkg, pvg, *refs):
    outs, (wide_sem, sem) = refs[:6], refs[6:]
    copies = [
        pltpu.make_async_copy(v.at[g], out.at[:, pl.ds(g * span, span)], wide_sem.at[i, g])
        for i, (v, out) in enumerate(((attn_v, outs[0]), (dq_v, outs[1])))
        for g in range(kv_heads)
    ] + [
        pltpu.make_async_copy(v, out, sem.at[i])
        for i, (v, out) in enumerate(zip((akg, avg, pkg, pvg), outs[2:]))
    ]
    for copy in copies:
        copy.start()
    for copy in copies:
        copy.wait()


def per_device(n, queries, answer_keys, answer_values, prompt_keys, prompt_values, out_grad, weights, lengths):
    height = queries.shape[0]
    d = HEAD_DIM
    columns = answer_keys.shape[1]
    kv_heads = columns // d
    group = queries.shape[1] // columns
    own_prompt = prompt_keys.shape[0]
    keys = own_prompt * n + 3 * height
    span = group * d
    bf16, f32 = jnp.bfloat16, jnp.float32
    vmem = pl.BlockSpec(memory_space=pltpu.VMEM)
    hbm = pl.BlockSpec(memory_space=pltpu.HBM)
    dma = pltpu.SemaphoreType.DMA
    results = pl.pallas_call(
        functools.partial(kernel, n, kv_heads, group),
        out_shape=(
            pltpu.VMEM((kv_heads, height, span), bf16),
            pltpu.VMEM((kv_heads, height, span), bf16),
            pltpu.VMEM(answer_keys.shape, bf16),
            pltpu.VMEM(answer_keys.shape, bf16),
            pltpu.VMEM(prompt_keys.shape, f32),
            pltpu.VMEM(prompt_keys.shape, f32),
        ),
        in_specs=[hbm, hbm] + [vmem] * 6,
        out_specs=(vmem,) * 6,
        scratch_shapes=[
            pltpu.VMEM((kv_heads, height, span), bf16),
            pltpu.VMEM((kv_heads, height, span), bf16),
            pltpu.VMEM((kv_heads, 2, 2, height, d), bf16),
            pltpu.VMEM((kv_heads, 2, own_prompt, d), bf16),
            pltpu.VMEM((kv_heads, 2, n // 2, 2, own_prompt, d), bf16),
            pltpu.VMEM((kv_heads, 2, n // 2, 2, own_prompt, d), f32),
            pltpu.VMEM((kv_heads, n // 2, 2, own_prompt, d), f32),
            pltpu.VMEM((kv_heads, n // 2, 2, own_prompt, d), bf16),
            pltpu.VMEM((kv_heads, n // 2, 2, own_prompt, d), bf16),
            pltpu.VMEM((kv_heads, 2, 2, height, d), bf16),
            pltpu.VMEM((kv_heads, 2, 2, height, d), bf16),
            pltpu.VMEM((kv_heads, 2, height, d), bf16),
            pltpu.VMEM((kv_heads, 2, height, d), bf16),
            pltpu.VMEM((kv_heads, 2, height, d), f32),
            pltpu.VMEM((group * height, d), bf16),
            pltpu.VMEM((group * height, d), bf16),
            pltpu.VMEM((keys, d), bf16),
            pltpu.VMEM((keys, d), bf16),
            pltpu.VMEM((d, keys), bf16),
            pltpu.VMEM((d, keys), bf16),
            pltpu.VMEM((keys, group * height), bf16),
            pltpu.VMEM((keys, group * height), bf16),
            pltpu.VMEM((2, height, height), f32),
            pltpu.VMEM((height, height), bf16),
            pltpu.VMEM((height, height), f32),
            dma((kv_heads, 2)),
            dma((kv_heads, 2)),
            dma((kv_heads, 2, 2)),
            dma((kv_heads, 2, 2)),
            dma((kv_heads, 2)),
            *[dma((kv_heads,))] * 10,
            dma((kv_heads, 2)),
            dma((kv_heads,)),
        ],
        compiler_params=pltpu.CompilerParams(
            collective_id=0, has_side_effects=True, vmem_limit_bytes=60 * 1024 * 1024
        ),
    )(
        queries, out_grad, answer_keys, answer_values, prompt_keys, prompt_values,
        weights.reshape(1, height), lengths.reshape(1, lengths.shape[0]),
    )
    return pl.pallas_call(
        functools.partial(write_out, kv_heads, span),
        out_shape=(
            jax.ShapeDtypeStruct(queries.shape, bf16),
            jax.ShapeDtypeStruct(queries.shape, bf16),
            jax.ShapeDtypeStruct(answer_keys.shape, bf16),
            jax.ShapeDtypeStruct(answer_keys.shape, bf16),
            jax.ShapeDtypeStruct(prompt_keys.shape, f32),
            jax.ShapeDtypeStruct(prompt_keys.shape, f32),
        ),
        in_specs=[vmem] * 6,
        out_specs=(hbm,) * 6,
        scratch_shapes=[dma((2, kv_heads)), dma((4,))],
        compiler_params=pltpu.CompilerParams(vmem_limit_bytes=4 * 1024 * 1024),
    )(*results)


def solution(mesh):
    both = ("grp", "row")
    wide = P(both, None)
    return jax.shard_map(
        functools.partial(per_device, mesh.shape["row"]),
        mesh=mesh,
        in_specs=(wide,) * 6 + (P(both), P("grp")),
        out_specs=(wide,) * 6,
        check_vma=False,
    )
```

```python
import functools
import math

import jax
import jax.numpy as jnp
from jax import lax
from jax.experimental import pallas as pl
from jax.experimental.pallas import tpu as pltpu
from jax.sharding import PartitionSpec as P

HEAD_DIM = 128
MASKED = -1e30
MESH = pl.DeviceIdType.MESH
NT = (((1,), (1,)), ((), ()))


def dot(a, b):
    return jnp.dot(a, b, preferred_element_type=jnp.float32)


def twice(x):
    return jnp.concatenate([x, x], axis=1)


def kernel(
    n, kv_heads, group,
    q_hbm, og_hbm, ak, av, pk, pv, w, lens,
    attn_v, dq_v, akg, avg, pkg, pvg,
    ogv, win, pst, pgath, psend, pmid, pred, precv,
    gsend, gmid, gout, grecv, own,
    qs, cots, cots_t, kcat, vcat, kt, vt, p_all, ds_all, bias, tri_b, wfull,
    in_sem, st_sem, win_send, win_recv, wr_send, pg_send, pg_recv, pp_send, pp_recv,
    pm_send, pm_recv, pr_send, pr_recv, gm_send, gm_recv, gr_send, gr_recv,
):
    me = lax.axis_index("row")
    height = ak.shape[0]
    d = HEAD_DIM
    span = group * d
    prompt = pk.shape[0] * n
    factor = d ** (-0.5)
    log_factor = factor * math.log2(math.e)

    chips = n // 2
    core = lax.rem(me, 2)
    chip = me // 2
    sibling = me + 1 - 2 * core
    across = lax.rem(me + n - 1 + 2 * core, n)

    def same(k):
        return lax.rem(me + 2 * k, n)

    def remote(src, dst, send, recv, target):
        return pltpu.make_async_remote_copy(
            src_ref=src, dst_ref=dst, send_sem=send, recv_sem=recv,
            device_id={"row": target}, device_id_type=MESH,
        )

    def cols(g, width):
        return pl.ds(pl.multiple_of(g * width, width), width)

    def q_copy(g, h):
        return pltpu.make_async_copy(
            q_hbm.at[:, pl.ds((g * group + h) * d, d)],
            qs.at[g, pl.ds(h * height, height)], in_sem.at[g, 0],
        )

    def og_copy(g):
        return pltpu.make_async_copy(og_hbm.at[:, cols(g, span)], ogv.at[g], in_sem.at[g, 1])

    def stage_copies(g):
        return (
            pltpu.make_async_copy(pk.at[:, cols(g, d)], pst.at[g, 0], st_sem.at[g, 0]),
            pltpu.make_async_copy(pv.at[:, cols(g, d)], pst.at[g, 1], st_sem.at[g, 1]),
        )

    def win_copy(g, far, which):
        return remote(
            (ak, av)[which].at[:, cols(g, d)], win.at[g, far, which],
            win_send.at[g, far, which], win_recv.at[g, far, which],
            same(1) if far else lax.rem(me + 1, n),
        )

    def win_relay(g, which):
        return remote(
            win.at[g, 0, which], win.at[g, 1, which],
            wr_send.at[g, which], win_recv.at[g, 1, which], sibling,
        )

    def gather_copy(g, k):
        return remote(
            pst.at[g], pgath.at[g, core, chip], pg_send.at[g], pg_recv.at[g], same(k)
        )

    def gather_relay(g):
        return remote(
            pgath.at[g, core], pgath.at[g, core], pp_send.at[g], pp_recv.at[g], sibling
        )

    def pair_copy(g):
        return remote(psend.at[g, 1 - core], pmid.at[g], pm_send.at[g], pm_recv.at[g], sibling)

    def reduce_copy(g, k):
        return remote(
            pred.at[g, lax.rem(chip + k, chips)], precv.at[g, chip],
            pr_send.at[g], pr_recv.at[g], same(k),
        )

    def mid_copy(g):
        return remote(gsend.at[g], gmid.at[g], gm_send.at[g], gm_recv.at[g], sibling)

    def back_copy(g, far):
        return remote(
            gsend.at[g, 1] if far else gout.at[g], grecv.at[g],
            gr_send.at[g, far], gr_recv.at[g], same(chips - 1) if far else across,
        )

    def relay(g):
        for which in range(2):
            win_copy(g, 0, which).wait_recv()

        @pl.when(core == 0)
        def _():
            for which in range(2):
                win_relay(g, which).start()

        here = pgath.at[g, core]
        pltpu.make_async_copy(here, here, pg_recv.at[g]).wait()
        gather_relay(g).start()

    def pass_on(g):
        pair_copy(g).wait_recv()
        pred[g] = (psend[g, core] + pmid[g]).astype(jnp.bfloat16)

        @pl.when(core == 0)
        def _():
            mid_copy(g).wait_recv()
            gout[g] = (
                gsend[g, 0].astype(jnp.float32) + gmid[g, 1].astype(jnp.float32)
            ).astype(jnp.bfloat16)
            own[g] = own[g] + gmid[g, 0].astype(jnp.float32)
            back_copy(g, 0).start()
            back_copy(g, 1).start()

        pltpu.make_async_copy(pred.at[g, chip], precv.at[g, chip], pr_recv.at[g]).start()

        @pl.loop(1, chips)
        def _(k):
            reduce_copy(g, k).start()

    barrier = pltpu.get_barrier_semaphore()

    @pl.loop(1, chips)
    def _(k):
        pl.semaphore_signal(barrier, inc=1, device_id={"row": same(k)}, device_id_type=MESH)

    for target in (sibling, across):
        pl.semaphore_signal(barrier, inc=1, device_id={"row": target}, device_id_type=MESH)

    for g in range(kv_heads):
        for copy in stage_copies(g):
            copy.start()
    for g in range(kv_heads):
        og_copy(g).start()
    for g in range(kv_heads):
        for h in range(group):
            q_copy(g, h).start()

    answers = lens.shape[1]
    row = lax.broadcasted_iota(jnp.int32, (answers, answers), 0)
    col = lax.broadcasted_iota(jnp.int32, (answers, answers), 1)
    starts = jnp.sum(
        jnp.where(col < row, jnp.broadcast_to(lens[...], (answers, answers)), 0),
        axis=1, keepdims=True,
    )
    pos = me * height + lax.broadcasted_iota(jnp.int32, (1, height), 1)
    first = jnp.max(jnp.where(starts <= pos, starts, 0), axis=0, keepdims=True)
    key = lax.broadcasted_iota(jnp.int32, (height, height), 0)
    query = lax.broadcasted_iota(jnp.int32, (height, height), 1)
    tri = key <= query
    base = me * height
    near = jnp.where(key + (base - height) >= first, 0.0, MASKED)
    both = jnp.where(tri, key + base, key + (base - 2 * height))
    both = jnp.where(both >= first, 0.0, MASKED)
    bias[0] = near
    bias[1] = both
    tri_b[...] = tri.astype(jnp.float32).astype(jnp.bfloat16)
    wfull[...] = jnp.broadcast_to(w[...], (height, height)).T

    def prepare(g):
        og_copy(g).wait()
        for h in range(group):
            rows = slice(h * height, (h + 1) * height)
            cot = wfull[...] * ogv[g, :, h * d : (h + 1) * d].astype(jnp.float32)
            cot = cot.astype(jnp.bfloat16)
            cots[g, rows, :] = cot
            cots_t[g, :, rows] = cot.T

    @pl.loop(0, kv_heads)
    def _(g):
        prepare(g)

    for g in range(kv_heads):
        for copy in stage_copies(g):
            copy.wait()
    pl.semaphore_wait(barrier, chips + 1)

    @pl.loop(0, kv_heads)
    def _(g):
        pltpu.make_async_copy(pst.at[g], pgath.at[g, core, chip], pg_recv.at[g]).start()

        @pl.loop(1, chips)
        def _(k):
            gather_copy(g, k).start()

        for which in range(2):
            win_copy(g, 0, which).start()

        @pl.when(core == 0)
        def _():
            for which in range(2):
                win_copy(g, 1, which).start()

    relay(0)

    @pl.loop(0, kv_heads)
    def _(g):
        mine = qs.at[g]
        pltpu.make_async_copy(mine, mine, in_sem.at[g, 0]).wait()
        there = pgath.at[g, 1 - core]
        pltpu.make_async_copy(there, there, pp_recv.at[g]).wait()
        for which in range(2):
            win_copy(g, 1, which).wait_recv()
        at1, at2, at3 = prompt, prompt + height, prompt + 2 * height
        for which, (cat, tr, mine) in enumerate(((kcat, kt, ak), (vcat, vt, av))):
            gathered = pgath[g, :, :, which].astype(jnp.float32).reshape(prompt, d)
            cat[:at1, :] = gathered.astype(jnp.bfloat16)
            cat[at1:at2, :] = win[g, 0, which]
            cat[at2:at3, :] = win[g, 1, which]
            cat[at3:, :] = mine[:, cols(g, d)]
            tr[...] = cat[...].T
        tri2 = twice(tri)
        for pair in range(group // 2):
            rows = slice(pair * 2 * height, (pair + 1) * 2 * height)
            s = lax.dot_general(kcat[...], qs[g, rows, :], NT, preferred_element_type=jnp.float32)
            s_p = s[:at1]
            s_1 = s[at1:at2] + twice(bias[0])
            s_c = jnp.where(tri2, s[at3:], s[at2:at3]) + twice(bias[1])
            top = jnp.maximum(
                jnp.maximum(jnp.max(s_p, axis=0, keepdims=True), jnp.max(s_1, axis=0, keepdims=True)),
                jnp.max(s_c, axis=0, keepdims=True),
            )
            e_p = jnp.exp2((s_p - top) * log_factor)
            e_1 = jnp.exp2((s_1 - top) * log_factor)
            e_c = jnp.exp2((s_c - top) * log_factor)
            total = (
                jnp.sum(e_p, axis=0, keepdims=True)
                + jnp.sum(e_1, axis=0, keepdims=True)
                + jnp.sum(e_c, axis=0, keepdims=True)
            )
            inv = 1.0 / total
            c_p, c_1, c_c = e_p * inv, e_1 * inv, e_c * inv
            trib2 = twice(tri_b[...])
            p_all[:at1, rows] = c_p.astype(jnp.bfloat16)
            p_all[at1:at2, rows] = c_1.astype(jnp.bfloat16)
            b_c = c_c.astype(jnp.bfloat16)
            b_d = b_c * trib2
            p_all[at2:at3, rows] = b_c - b_d
            p_all[at3:, rows] = b_d
            out_t = dot(vt[...], p_all[:, rows]).astype(jnp.bfloat16)
            cot_t = cots_t[g, :, rows]
            delta = jnp.sum(
                cot_t.astype(jnp.float32) * out_t.astype(jnp.float32), axis=0, keepdims=True
            )
            slopes = dot(vcat[...], cot_t)
            ds_all[:at1, rows] = (c_p * (slopes[:at1] - delta)).astype(jnp.bfloat16)
            ds_all[at1:at2, rows] = (c_1 * (slopes[at1:at2] - delta)).astype(jnp.bfloat16)
            s_c = jnp.where(tri2, slopes[at3:], slopes[at2:at3])
            g_c = (c_c * (s_c - delta)).astype(jnp.bfloat16)
            g_d = g_c * trib2
            ds_all[at2:at3, rows] = g_c - g_d
            ds_all[at3:, rows] = g_d
            out = out_t.T
            for j in range(2):
                lanes = slice((2 * pair + j) * d, (2 * pair + j + 1) * d)
                attn_v[g, :, lanes] = out[j * height : (j + 1) * height]
        for which in range(2):
            if which == 0:
                part = dot(ds_all[...], qs[g]) * factor
            else:
                part = dot(p_all[...], cots[g])
            psend[g, :, :, which] = part[:at1].reshape(2, chips, prompt // n, d)
            gsend[g, 0, which] = part[at1:at2].astype(jnp.bfloat16)
            gsend[g, 1, which] = part[at2:at3].astype(jnp.bfloat16)
            own[g, which] = part[at3:]
        pair_copy(g).start()

        @pl.when(core == 1)
        def _():
            mid_copy(g).start()

        @pl.when(g < kv_heads - 1)
        def _():
            relay(g + 1)

        dq_t = (dot(kt[...], ds_all[...]) * factor).astype(jnp.bfloat16)
        for h in range(group):
            rows = slice(h * height, (h + 1) * height)
            dq_v[g, :, h * d : (h + 1) * d] = dq_t[:, rows].T
        pass_on(g)

    for g in range(kv_heads):
        lanes = slice(g * d, (g + 1) * d)
        back_copy(g, 0).wait_recv()
        for which, grad in enumerate((akg, avg)):
            grad[:, lanes] = (own[g, which] + grecv[g, which].astype(jnp.float32)).astype(
                jnp.bfloat16
            )
        pltpu.make_async_copy(precv.at[g], precv.at[g], pr_recv.at[g]).wait()
        for which, grad in enumerate((pkg, pvg)):
            grad[:, lanes] = jnp.sum(precv[g, :, which].astype(jnp.float32), axis=0)

    for g in range(kv_heads):
        pair_copy(g).wait_send()
        gather_relay(g).wait_send()
        for which in range(2):
            win_copy(g, 0, which).wait_send()
        sent = pgath.at[g, 0, pl.ds(0, chips - 1)]
        pltpu.make_async_copy(sent, sent, pg_send.at[g]).wait()
        sent = precv.at[g, pl.ds(0, chips - 1)]
        pltpu.make_async_copy(sent, sent, pr_send.at[g]).wait()

        @pl.when(core == 0)
        def _():
            for which in range(2):
                win_copy(g, 1, which).wait_send()
                win_relay(g, which).wait_send()
                back_copy(g, which).wait_send()

        @pl.when(core == 1)
        def _():
            mid_copy(g).wait_send()


def write_out(kv_heads, span, attn_v, dq_v, akg, avg, pkg, pvg, *refs):
    outs, (wide_sem, sem) = refs[:6], refs[6:]
    copies = [
        pltpu.make_async_copy(v.at[g], out.at[:, pl.ds(g * span, span)], wide_sem.at[i, g])
        for i, (v, out) in enumerate(((attn_v, outs[0]), (dq_v, outs[1])))
        for g in range(kv_heads)
    ] + [
        pltpu.make_async_copy(v, out, sem.at[i])
        for i, (v, out) in enumerate(zip((akg, avg, pkg, pvg), outs[2:]))
    ]
    for copy in copies:
        copy.start()
    for copy in copies:
        copy.wait()


def per_device(n, queries, answer_keys, answer_values, prompt_keys, prompt_values, out_grad, weights, lengths):
    height = queries.shape[0]
    d = HEAD_DIM
    columns = answer_keys.shape[1]
    kv_heads = columns // d
    group = queries.shape[1] // columns
    own_prompt = prompt_keys.shape[0]
    keys = own_prompt * n + 3 * height
    span = group * d
    bf16, f32 = jnp.bfloat16, jnp.float32
    vmem = pl.BlockSpec(memory_space=pltpu.VMEM)
    hbm = pl.BlockSpec(memory_space=pltpu.HBM)
    dma = pltpu.SemaphoreType.DMA
    results = pl.pallas_call(
        functools.partial(kernel, n, kv_heads, group),
        out_shape=(
            pltpu.VMEM((kv_heads, height, span), bf16),
            pltpu.VMEM((kv_heads, height, span), bf16),
            pltpu.VMEM(answer_keys.shape, bf16),
            pltpu.VMEM(answer_keys.shape, bf16),
            pltpu.VMEM(prompt_keys.shape, f32),
            pltpu.VMEM(prompt_keys.shape, f32),
        ),
        in_specs=[hbm, hbm] + [vmem] * 6,
        out_specs=(vmem,) * 6,
        scratch_shapes=[
            pltpu.VMEM((kv_heads, height, span), bf16),
            pltpu.VMEM((kv_heads, 2, 2, height, d), bf16),
            pltpu.VMEM((kv_heads, 2, own_prompt, d), bf16),
            pltpu.VMEM((kv_heads, 2, n // 2, 2, own_prompt, d), bf16),
            pltpu.VMEM((kv_heads, 2, n // 2, 2, own_prompt, d), f32),
            pltpu.VMEM((kv_heads, n // 2, 2, own_prompt, d), f32),
            pltpu.VMEM((kv_heads, n // 2, 2, own_prompt, d), bf16),
            pltpu.VMEM((kv_heads, n // 2, 2, own_prompt, d), bf16),
            pltpu.VMEM((kv_heads, 2, 2, height, d), bf16),
            pltpu.VMEM((kv_heads, 2, 2, height, d), bf16),
            pltpu.VMEM((kv_heads, 2, height, d), bf16),
            pltpu.VMEM((kv_heads, 2, height, d), bf16),
            pltpu.VMEM((kv_heads, 2, height, d), f32),
            pltpu.VMEM((kv_heads, group * height, d), bf16),
            pltpu.VMEM((kv_heads, group * height, d), bf16),
            pltpu.VMEM((kv_heads, d, group * height), bf16),
            pltpu.VMEM((keys, d), bf16),
            pltpu.VMEM((keys, d), bf16),
            pltpu.VMEM((d, keys), bf16),
            pltpu.VMEM((d, keys), bf16),
            pltpu.VMEM((keys, group * height), bf16),
            pltpu.VMEM((keys, group * height), bf16),
            pltpu.VMEM((2, height, height), f32),
            pltpu.VMEM((height, height), bf16),
            pltpu.VMEM((height, height), f32),
            dma((kv_heads, 2)),
            dma((kv_heads, 2)),
            dma((kv_heads, 2, 2)),
            dma((kv_heads, 2, 2)),
            dma((kv_heads, 2)),
            *[dma((kv_heads,))] * 10,
            dma((kv_heads, 2)),
            dma((kv_heads,)),
        ],
        compiler_params=pltpu.CompilerParams(
            collective_id=0, has_side_effects=True, vmem_limit_bytes=60 * 1024 * 1024
        ),
    )(
        queries, out_grad, answer_keys, answer_values, prompt_keys, prompt_values,
        weights.reshape(1, height), lengths.reshape(1, lengths.shape[0]),
    )
    return pl.pallas_call(
        functools.partial(write_out, kv_heads, span),
        out_shape=(
            jax.ShapeDtypeStruct(queries.shape, bf16),
            jax.ShapeDtypeStruct(queries.shape, bf16),
            jax.ShapeDtypeStruct(answer_keys.shape, bf16),
            jax.ShapeDtypeStruct(answer_keys.shape, bf16),
            jax.ShapeDtypeStruct(prompt_keys.shape, f32),
            jax.ShapeDtypeStruct(prompt_keys.shape, f32),
        ),
        in_specs=[vmem] * 6,
        out_specs=(hbm,) * 6,
        scratch_shapes=[dma((2, kv_heads)), dma((4,))],
        compiler_params=pltpu.CompilerParams(vmem_limit_bytes=4 * 1024 * 1024),
    )(*results)


def solution(mesh):
    both = ("grp", "row")
    wide = P(both, None)
    return jax.shard_map(
        functools.partial(per_device, mesh.shape["row"]),
        mesh=mesh,
        in_specs=(wide,) * 6 + (P(both), P("grp")),
        out_specs=(wide,) * 6,
        check_vma=False,
    )
```
